8 devices in a mesh: dp: 2 (over z, y), tp: 4 (over x, core).
Axes of the slice: x: 2, y: 2, z: 1, core: 2. Of those that a mesh axis runs over, the one named last changes fastest.
Arguments:
- hidden: bfloat16 [6, 512, 896], P('dp')
- norm_w: bfloat16 [896], replicated
- embed_table: bfloat16 [151936, 896], P('tp')
- labels: int32 [6, 512], P('dp')
- loss_mask: int32 [6, 512], P('dp')
Outputs:
- output 1: float32 [], replicated
- output 2: bfloat16 [6, 512, 896], P('dp')
- output 3: float32 [896], replicated
- output 4: float32 [151936, 896], P('tp')
All inputs are finite; a program needn't handle non-finite values.
Results may differ from the reference program's by a relative error of at most 0.001.
Values sent between devices are 32-bit elements.
A program may use at most 1 GiB of HBM per device.

```python
import math
import jax
import jax.numpy as jnp
from jax import lax

BATCH_ROWS = 6
SEQ_LEN = 512
MODEL_DIM = 896
VOCAB_SIZE = 151936
TOKEN_BLOCK = 128
SOFT_CAP = 30.0


def draw_labels(root_key):
    key_pick, key_common, key_any = jax.random.split(root_key, 3)
    label_shape = (BATCH_ROWS, SEQ_LEN)
    pick_val = jax.random.randint(key_pick, label_shape, 0, 4)
    common_id = jax.random.randint(key_common, label_shape, 0, VOCAB_SIZE // 32)
    any_id = jax.random.randint(key_any, label_shape, 0, VOCAB_SIZE)
    return jnp.where(pick_val == 0, any_id, common_id).astype(jnp.int32)


def draw_mask(root_key):
    key_rate, key_roll = jax.random.split(root_key, 2)
    drop_pct = jax.random.randint(key_rate, (BATCH_ROWS, 1), 5, 40)
    roll_val = jax.random.randint(key_roll, (BATCH_ROWS, SEQ_LEN), 0, 100)
    return (roll_val >= drop_pct).astype(jnp.int32)


def norm_apply(hid_rows, gain32):
    h32 = hid_rows.astype(jnp.float32)
    inv_rms = lax.rsqrt(jnp.mean(h32 * h32, axis=-1, keepdims=True) + 1e-6)
    return h32 * inv_rms * (1.0 + gain32)


def setup_inputs(seed: int = 0) -> dict:
    root_key = jax.random.key(seed)
    key_noise, key_gain, key_table, key_str, key_lab, key_mask, key_top = jax.random.split(root_key, 7)
    table_scale = 3.0 / math.sqrt(MODEL_DIM)
    table32 = jax.random.normal(key_table, (VOCAB_SIZE, MODEL_DIM), jnp.float32) * table_scale
    labels = draw_labels(key_lab)
    top_str = jax.random.uniform(key_top, (), jnp.float32, minval=3.0, maxval=6.5)
    strength = jax.random.uniform(key_str, (BATCH_ROWS, SEQ_LEN, 1), jnp.float32) * top_str
    noise_val = jax.random.normal(key_noise, (BATCH_ROWS, SEQ_LEN, MODEL_DIM), jnp.float32)
    hidden = noise_val + strength * jnp.take(table32, labels, axis=0)
    gain_vec = 0.3 * jax.random.normal(key_gain, (MODEL_DIM,), jnp.float32)
    return {'hidden': hidden.astype(jnp.bfloat16), 'norm_w': gain_vec.astype(jnp.bfloat16), 'embed_table': table32.astype(jnp.bfloat16), 'labels': labels, 'loss_mask': draw_mask(key_mask)}


def reference(hidden, norm_w, embed_table, labels, loss_mask):
    tokens = BATCH_ROWS * SEQ_LEN
    n_blocks = tokens // TOKEN_BLOCK
    hid_blocks = hidden.reshape(n_blocks, TOKEN_BLOCK, MODEL_DIM)
    lab_blocks = labels.reshape(n_blocks, TOKEN_BLOCK)
    mask_blocks = loss_mask.reshape(n_blocks, TOKEN_BLOCK).astype(jnp.float32)
    tok_count = jnp.maximum(jnp.sum(mask_blocks), 1.0)
    gain32 = norm_w.astype(jnp.float32)
    vocab_ids = jnp.arange(VOCAB_SIZE, dtype=jnp.int32)

    def block_step(carry_in, block_in):
        loss_sum, grad_gain, grad_table = carry_in
        hid_rows, lab_rows, mask_rows = block_in
        normed, norm_back = jax.vjp(norm_apply, hid_rows, gain32)
        normed_bf = normed.astype(jnp.bfloat16)
        logits = jnp.dot(normed_bf, embed_table.T, preferred_element_type=jnp.float32)
        capped = SOFT_CAP * jnp.tanh(logits / SOFT_CAP)
        row_max = jnp.max(capped, axis=-1, keepdims=True)
        exp_shift = jnp.exp(capped - row_max)
        row_sum = jnp.sum(exp_shift, axis=-1, keepdims=True)
        onehot = vocab_ids[None, :] == lab_rows[:, None]
        picked = jnp.sum(jnp.where(onehot, capped, 0.0), axis=-1)
        tok_loss = jnp.log(row_sum[:, 0]) + row_max[:, 0] - picked
        tok_scale = mask_rows / tok_count
        cap_ratio = capped / SOFT_CAP
        grad_logit = ((exp_shift / row_sum - onehot.astype(jnp.float32)) * tok_scale[:, None] * (1.0 - cap_ratio * cap_ratio)).astype(jnp.bfloat16)
        grad_x = jnp.dot(grad_logit, embed_table, preferred_element_type=jnp.float32)
        grad_rows, grad_g = norm_back(grad_x)
        table_part = jnp.dot(grad_logit.T, normed_bf, preferred_element_type=jnp.float32)
        new_carry = (loss_sum + jnp.sum(mask_rows * tok_loss), grad_gain + grad_g, grad_table + table_part)
        return new_carry, grad_rows

    init_carry = (jnp.zeros((), jnp.float32), jnp.zeros((MODEL_DIM,), jnp.float32), jnp.zeros((VOCAB_SIZE, MODEL_DIM), jnp.float32))
    final_carry, grad_rows = lax.scan(block_step, init_carry, (hid_blocks, lab_blocks, mask_blocks))
    loss_sum, grad_gain, grad_table = final_carry
    return loss_sum / tok_count, grad_rows.reshape(BATCH_ROWS, SEQ_LEN, MODEL_DIM), grad_gain, grad_table
```

```python
import functools
import jax
import jax.numpy as jnp
from jax import lax
from jax.experimental import pallas as pl
from jax.experimental.pallas import tpu as pltpu
from jax.sharding import PartitionSpec as P

SOFT_CAP = 30.0
LOG2E = 1.4426950408889634
CAP2 = SOFT_CAP * LOG2E
VMEM_LIMIT = 60 * 1024 * 1024


def norm_apply(hid_rows, gain32):
    h32 = hid_rows.astype(jnp.float32)
    inv_rms = lax.rsqrt(jnp.mean(h32 * h32, axis=-1, keepdims=True) + 1e-6)
    return h32 * inv_rms * (1.0 + gain32)


def chunks(total, size):
    return [(s, min(size, total - s)) for s in range(0, total, size)]


def per_block(nblk, rows, tail, body):
    if tail == 0:
        body(rows)
        return
    i = pl.program_id(0)

    @pl.when(i < nblk - 1)
    def _():
        body(rows)

    @pl.when(i == nblk - 1)
    def _():
        body(tail)


def row_hits(rows, cols, base, labels):
    ids = lax.broadcasted_iota(jnp.int32, (rows, cols), 0)
    return ids == (labels - base)


def logits_kernel(nblk, bv, tail, e_ref, xt_ref, lab_ref, t_ref, sum_ref, pick_ref):
    i = pl.program_id(0)

    @pl.when(i == 0)
    def _():
        sum_ref[...] = jnp.zeros_like(sum_ref)
        pick_ref[...] = jnp.zeros_like(pick_ref)

    tokens = xt_ref.shape[1]

    def body(rows):
        for m, mm in chunks(rows, 256):
            for n, nn in chunks(tokens, 512):
                cols = slice(n, n + nn)
                z = jnp.dot(e_ref[m:m + mm, :], xt_ref[:, cols], preferred_element_type=jnp.float32)
                t = jnp.tanh(z * (1.0 / SOFT_CAP))
                t_ref[m:m + mm, cols] = t
                e = jnp.exp2(t * CAP2)
                sum_ref[:, cols] += jnp.sum(e.reshape(mm // 8, 8, nn), axis=0)
                hit = row_hits(mm, nn, i * bv + m, lab_ref[:, cols])
                pick_ref[:, cols] += jnp.sum(jnp.where(hit, t, 0.0).reshape(mm // 8, 8, nn), axis=0)

    per_block(nblk, bv, tail, body)


def grad_of(t, base, lab, lz, ts):
    p = jnp.exp2(t * CAP2 - lz)
    hit = row_hits(t.shape[0], t.shape[1], base, lab)
    return (jnp.where(hit, p - 1.0, p) * ts * (1.0 - t * t)).astype(jnp.bfloat16)


def grad_x_kernel(nblk, bv, tail, e_ref, t_ref, lab_ref, lz_ref, ts_ref, gx_ref, et_ref, g_ref):
    i = pl.program_id(0)

    @pl.when(i == 0)
    def _():
        gx_ref[...] = jnp.zeros_like(gx_ref)

    tokens = t_ref.shape[1]

    def body(rows):
        for m, mm in chunks(rows, 256):
            et_ref[:, m:m + mm] = e_ref[m:m + mm, :].T
        for n, nn in chunks(tokens, 512):
            cols = slice(n, n + nn)
            for m, mm in chunks(rows, 64):
                g_ref[m:m + mm, cols] = grad_of(
                    t_ref[m:m + mm, cols], i * bv + m, lab_ref[:, cols], lz_ref[:, cols], ts_ref[:, cols])
            gx_ref[:, cols] += jnp.dot(et_ref[:, :rows], g_ref[:rows, cols], preferred_element_type=jnp.float32)

    per_block(nblk, bv, tail, body)


def grad_table_kernel(nblk, bv, tail, e_ref, t_ref, xto_ref, xs_ref, xo_ref, lab_ref, lz_ref, ts_ref, de_ref, g_ref, go_ref):
    i = pl.program_id(0)
    tokens = t_ref.shape[1]

    def body(rows):
        for n, nn in chunks(tokens, 512):
            cols = slice(n, n + nn)
            for m, mm in chunks(rows, 64):
                g_ref[m:m + mm, cols] = grad_of(
                    t_ref[m:m + mm, cols], i * bv + m, lab_ref[0:1, cols], lz_ref[0:1, cols], ts_ref[0:1, cols])
            for m, mm in chunks(rows, 256):
                z = jnp.dot(e_ref[m:m + mm, :], xto_ref[:, cols], preferred_element_type=jnp.float32)
                t = jnp.tanh(z * (1.0 / SOFT_CAP))
                go_ref[m:m + mm, cols] = grad_of(
                    t, i * bv + m, lab_ref[1:2, cols], lz_ref[1:2, cols], ts_ref[1:2, cols])
        part = jnp.dot(g_ref[:rows, :], xs_ref[...], preferred_element_type=jnp.float32)
        de_ref[:rows, :] = part + jnp.dot(go_ref[:rows, :], xo_ref[...], preferred_element_type=jnp.float32)

    per_block(nblk, bv, tail, body)


def prep_kernel(x32_ref, x_ref, xt_ref):
    x = x32_ref[...].astype(jnp.bfloat16)
    x_ref[...] = x
    xt_ref[...] = x.T


def whole(shape):
    return pl.BlockSpec(shape, lambda *_: (0,) * len(shape))


def params():
    return pltpu.CompilerParams(dimension_semantics=("arbitrary",), vmem_limit_bytes=VMEM_LIMIT)


def solution(mesh):
    n_dp = mesh.shape['dp']
    swap = [(i, n_dp - 1 - i) for i in range(n_dp)]

    def local_step(hidden, norm_w, embed_table, labels, loss_mask):
        batch_rows, seq_len, dim = hidden.shape
        vocab = embed_table.shape[0]
        tokens = batch_rows * seq_len
        hid_rows = hidden.reshape(tokens, dim)
        mask_own = loss_mask.reshape(1, tokens).astype(jnp.float32)
        normed, norm_back = jax.vjp(norm_apply, hid_rows, norm_w.astype(jnp.float32))
        x_own = normed.astype(jnp.bfloat16)
        other32 = lax.ppermute(normed, 'dp', swap)
        base = lax.axis_index('tp') * vocab
        lab_own = labels.reshape(1, tokens) - base
        lab_other = lax.ppermute(labels.reshape(1, tokens), 'dp', swap) - base

        bv = 1024
        nblk = pl.cdiv(vocab, bv)
        tail = vocab % bv
        row = whole((1, tokens))
        row2 = whole((2, tokens))
        e_spec = pl.BlockSpec((bv, dim), lambda i: (i, 0))
        t_spec = pl.BlockSpec((bv, tokens), lambda i: (i, 0))
        flops = 2 * tokens * vocab * dim
        t_own, sums, picks = pl.pallas_call(
            functools.partial(logits_kernel, nblk, bv, tail),
            grid=(nblk,),
            in_specs=[e_spec, whole((dim, tokens)), row],
            out_specs=[t_spec, whole((8, tokens)), whole((8, tokens))],
            out_shape=[jax.ShapeDtypeStruct((vocab, tokens), jnp.float32)]
            + [jax.ShapeDtypeStruct((8, tokens), jnp.float32)] * 2,
            compiler_params=params(),
            cost_estimate=pl.CostEstimate(flops=flops, bytes_accessed=vocab * (tokens * 4 + dim * 2), transcendentals=2 * vocab * tokens),
            name="logits",
        )(embed_table, x_own.T, lab_own)

        stat = jnp.stack([jnp.sum(sums, axis=0), jnp.sum(picks, axis=0)])
        stat = lax.psum(stat, 'tp')
        pack_own = jnp.concatenate([stat, mask_own], axis=0)
        pack_other = lax.ppermute(pack_own, 'dp', swap)
        z_both = jnp.stack([pack_own[0], pack_other[0]])
        pick_both = jnp.stack([pack_own[1], pack_other[1]]) * SOFT_CAP
        mask_both = jnp.stack([pack_own[2], pack_other[2]])
        tok_count = jnp.maximum(jnp.sum(mask_both), 1.0)
        mean_loss = jnp.sum(mask_both * (jnp.log(z_both) - pick_both)) / tok_count
        lz = jnp.log2(z_both)
        ts = mask_both / tok_count
        lab = jnp.concatenate([lab_own, lab_other], axis=0)

        gxt = pl.pallas_call(
            functools.partial(grad_x_kernel, nblk, bv, tail),
            grid=(nblk,),
            in_specs=[e_spec, t_spec, row, row, row],
            out_specs=whole((dim, tokens)),
            out_shape=jax.ShapeDtypeStruct((dim, tokens), jnp.float32),
            scratch_shapes=[pltpu.VMEM((dim, bv), jnp.bfloat16), pltpu.VMEM((bv, tokens), jnp.bfloat16)],
            compiler_params=params(),
            cost_estimate=pl.CostEstimate(flops=flops, bytes_accessed=vocab * (tokens * 4 + dim * 2), transcendentals=vocab * tokens),
            name="grad_x",
        )(embed_table, t_own, lab_own, lz[0:1], ts[0:1])
        grad_x = lax.psum(gxt, 'tp').T

        x_other, xt_other = pl.pallas_call(
            prep_kernel,
            out_shape=[jax.ShapeDtypeStruct((tokens, dim), jnp.bfloat16), jax.ShapeDtypeStruct((dim, tokens), jnp.bfloat16)],
            compiler_params=pltpu.CompilerParams(vmem_limit_bytes=VMEM_LIMIT),
            name="prep_other",
        )(other32)

        bt = 512
        nblk_t = pl.cdiv(vocab, bt)
        tail_t = vocab % bt
        grad_table = pl.pallas_call(
            functools.partial(grad_table_kernel, nblk_t, bt, tail_t),
            grid=(nblk_t,),
            in_specs=[
                pl.BlockSpec((bt, dim), lambda i: (i, 0)), pl.BlockSpec((bt, tokens), lambda i: (i, 0)),
                whole((dim, tokens)), whole((tokens, dim)), whole((tokens, dim)), row2, row2, row2],
            out_specs=pl.BlockSpec((bt, dim), lambda i: (i, 0)),
            out_shape=jax.ShapeDtypeStruct((vocab, dim), jnp.float32),
            scratch_shapes=[pltpu.VMEM((bt, tokens), jnp.bfloat16), pltpu.VMEM((bt, tokens), jnp.bfloat16)],
            compiler_params=params(),
            cost_estimate=pl.CostEstimate(flops=3 * flops, bytes_accessed=vocab * (tokens * 4 + dim * 6), transcendentals=3 * vocab * tokens),
            name="grad_table",
        )(embed_table, t_own, xt_other, x_own, x_other, lab, lz, ts)

        grad_rows, grad_gain = norm_back(grad_x)
        grad_gain = lax.psum(grad_gain, 'dp')
        return mean_loss, grad_rows.reshape(batch_rows, seq_len, dim), grad_gain, grad_table

    return jax.shard_map(local_step, mesh=mesh, in_specs=(P('dp', None, None), P(None), P('tp', None), P('dp', None), P('dp', None)), out_specs=(P(), P('dp', None, None), P(None), P('tp', None)), check_vma=False)
```

```python
import functools
import jax
import jax.numpy as jnp
from jax import lax
from jax.experimental import pallas as pl
from jax.experimental.pallas import tpu as pltpu
from jax.sharding import PartitionSpec as P

SOFT_CAP = 30.0
LOG2E = 1.4426950408889634
CAP2 = SOFT_CAP * LOG2E
VMEM_LIMIT = 60 * 1024 * 1024
TILE = 256


def norm_apply(hid_rows, gain32):
    h32 = hid_rows.astype(jnp.float32)
    inv_rms = lax.rsqrt(jnp.mean(h32 * h32, axis=-1, keepdims=True) + 1e-6)
    return h32 * inv_rms * (1.0 + gain32)


def chunks(total, size):
    return [(s, min(size, total - s)) for s in range(0, total, size)]


def per_width(n_tiles, tokens, body):
    full = tokens // TILE
    widths = list(range(max(1, full - 2), full + 1))
    for k, w in enumerate(widths):
        if len(widths) == 1:
            cond = True
        elif k == 0:
            cond = n_tiles <= w
        elif k == len(widths) - 1:
            cond = n_tiles >= w
        else:
            cond = n_tiles == w

        @pl.when(cond)
        def _():
            body(w * TILE)


def row_hits(rows, cols, base, labels):
    ids = lax.broadcasted_iota(jnp.int32, (rows, cols), 0)
    return ids == (labels - base)


def prep_kernel(hid_ref, mask_ref, dig_ref, gain_ref, hc_ref, x_ref, xt_ref, x32_ref, perm_ref, lab_ref):
    tokens = hid_ref.shape[0]
    mask = mask_ref[...]
    src = lax.broadcasted_iota(jnp.int32, (tokens, tokens), 0)
    dst = lax.broadcasted_iota(jnp.int32, (tokens, tokens), 1)
    upto = jnp.where(src <= dst, 1.0, 0.0).astype(jnp.bfloat16)
    count = jnp.dot(jnp.broadcast_to(mask, (8, tokens)).astype(jnp.bfloat16), upto, preferred_element_type=jnp.float32)
    place = jnp.where(mask > 0.0, count[0:1, :] - 1.0, -1.0).astype(jnp.int32)
    perm_ref[...] = jnp.where(src == place, 1.0, 0.0).astype(jnp.bfloat16)
    hc_ref[...] = jnp.dot(perm_ref[...], hid_ref[...], preferred_element_type=jnp.float32).astype(jnp.bfloat16)
    digits = lax.dot_general(dig_ref[...], perm_ref[...], (((1,), (1,)), ((), ())), preferred_element_type=jnp.float32)
    lab_ref[...] = digits[0:1, :] + 64.0 * digits[1:2, :] + 4096.0 * digits[2:3, :]
    for m, mm in chunks(tokens, TILE):
        rows = slice(m, m + mm)
        x32 = norm_apply(hc_ref[rows, :], gain_ref[...])
        x = x32.astype(jnp.bfloat16)
        x32_ref[rows, :] = x32
        x_ref[rows, :] = x
        xt_ref[:, rows] = x.T


def other_kernel(x32_ref, x_ref, xt_ref):
    x = x32_ref[...].astype(jnp.bfloat16)
    x_ref[...] = x
    xt_ref[...] = x.T


def logits_kernel(nblk, bv, tail, nt_ref, e_ref, xt_ref, lab_ref, t_ref, sum_ref, pick_ref):
    i = pl.program_id(0)
    tokens = xt_ref.shape[1]

    @pl.when(i == 0)
    def _():
        sum_ref[...] = jnp.zeros_like(sum_ref)
        pick_ref[...] = jnp.zeros_like(pick_ref)

    def body(rows, width):
        for m, mm in chunks(rows, 256):
            for n, nn in chunks(width, 512):
                cols = slice(n, n + nn)
                z = jnp.dot(e_ref[m:m + mm, :], xt_ref[:, cols], preferred_element_type=jnp.float32)
                t = jnp.tanh(z * (1.0 / SOFT_CAP))
                t_ref[m:m + mm, cols] = t
                e = jnp.exp2(t * CAP2)
                sum_ref[:, cols] += jnp.sum(e.reshape(mm // 8, 8, nn), axis=0)
                hit = row_hits(mm, nn, i * bv + m, lab_ref[:, cols])
                pick_ref[:, cols] += jnp.sum(jnp.where(hit, t, 0.0).reshape(mm // 8, 8, nn), axis=0)

    @pl.when(i < nblk - 1)
    def _():
        per_width(nt_ref[0], tokens, functools.partial(body, bv))

    @pl.when(i == nblk - 1)
    def _():
        body(tail, tokens)


def grad_of(t, base, lab, lz, ts):
    p = jnp.exp2(t * CAP2 - lz)
    hit = row_hits(t.shape[0], t.shape[1], base, lab)
    return (jnp.where(hit, p - 1.0, p) * ts * (1.0 - t * t)).astype(jnp.bfloat16)


def grad_x_kernel(nblk, bv, tail, nt_ref, e_ref, t_ref, lab_ref, lz_ref, ts_ref, gx_ref, et_ref, g_ref):
    i = pl.program_id(0)
    tokens = t_ref.shape[1]

    @pl.when(i == 0)
    def _():
        gx_ref[...] = jnp.zeros_like(gx_ref)

    def body(rows, width):
        for m, mm in chunks(rows, 256):
            et_ref[:, m:m + mm] = e_ref[m:m + mm, :].T
        for n, nn in chunks(width, 512):
            cols = slice(n, n + nn)
            for m, mm in chunks(rows, 64):
                g_ref[m:m + mm, cols] = grad_of(
                    t_ref[m:m + mm, cols], i * bv + m, lab_ref[:, cols], lz_ref[:, cols], ts_ref[:, cols])
            gx_ref[:, cols] += jnp.dot(et_ref[:, :rows], g_ref[:rows, cols], preferred_element_type=jnp.float32)

    @pl.when(i < nblk - 1)
    def _():
        per_width(nt_ref[0], tokens, functools.partial(body, bv))

    @pl.when(i == nblk - 1)
    def _():
        body(tail, tokens)


def grad_table_kernel(nblk, bv, tail, nt_ref, e_ref, t_ref, xto_ref, xs_ref, xo_ref, lab_ref, lz_ref, ts_ref, de_ref, g_ref):
    i = pl.program_id(0)
    tokens = t_ref.shape[1]

    def own(rows, width):
        for n, nn in chunks(width, 512):
            cols = slice(n, n + nn)
            for m, mm in chunks(rows, 64):
                g_ref[m:m + mm, cols] = grad_of(
                    t_ref[m:m + mm, cols], i * bv + m, lab_ref[0:1, cols], lz_ref[0:1, cols], ts_ref[0:1, cols])
        de_ref[:rows, :] = jnp.dot(g_ref[:rows, :width], xs_ref[:width, :], preferred_element_type=jnp.float32)

    def other(rows, width):
        for n, nn in chunks(width, 512):
            cols = slice(n, n + nn)
            for m, mm in chunks(rows, 256):
                z = jnp.dot(e_ref[m:m + mm, :], xto_ref[:, cols], preferred_element_type=jnp.float32)
                t = jnp.tanh(z * (1.0 / SOFT_CAP))
                g_ref[m:m + mm, cols] = grad_of(
                    t, i * bv + m, lab_ref[1:2, cols], lz_ref[1:2, cols], ts_ref[1:2, cols])
        de_ref[:rows, :] += jnp.dot(g_ref[:rows, :width], xo_ref[:width, :], preferred_element_type=jnp.float32)

    @pl.when(i < nblk - 1)
    def _():
        per_width(nt_ref[0], tokens, functools.partial(own, bv))
        per_width(nt_ref[1], tokens, functools.partial(other, bv))

    @pl.when(i == nblk - 1)
    def _():
        own(tail, tokens)
        other(tail, tokens)


def whole(shape):
    return pl.BlockSpec(shape, lambda *_: (0,) * len(shape))


def blocks(rows, cols):
    return pl.BlockSpec((rows, cols), lambda i, *_: (i, 0))


def params(**kw):
    return pltpu.CompilerParams(vmem_limit_bytes=VMEM_LIMIT, **kw)


def table_call(kernel, vocab, rows, in_specs, out_specs, out_shape, scratch, cost):
    nblk = pl.cdiv(vocab, rows)
    tail = vocab - (nblk - 1) * rows
    return pl.pallas_call(
        functools.partial(kernel, nblk, rows, tail),
        grid_spec=pltpu.PrefetchScalarGridSpec(
            num_scalar_prefetch=1, grid=(nblk,), in_specs=in_specs, out_specs=out_specs, scratch_shapes=scratch),
        out_shape=out_shape,
        compiler_params=params(dimension_semantics=("arbitrary",)),
        cost_estimate=cost,
    )


def solution(mesh):
    n_dp = mesh.shape['dp']
    swap = [(i, n_dp - 1 - i) for i in range(n_dp)]

    def local_step(hidden, norm_w, embed_table, labels, loss_mask):
        batch_rows, seq_len, dim = hidden.shape
        vocab = embed_table.shape[0]
        tokens = batch_rows * seq_len
        hid_rows = hidden.reshape(tokens, dim)
        mask_rows = loss_mask.reshape(1, tokens).astype(jnp.float32)
        gain = norm_w.astype(jnp.float32)
        lab_rows = labels.reshape(tokens)
        digits = jnp.stack([lab_rows & 63, (lab_rows >> 6) & 63, lab_rows >> 12] + [jnp.zeros_like(lab_rows)] * 5)
        f32, b16 = jnp.float32, jnp.bfloat16
        shape = jax.ShapeDtypeStruct
        hid_c, x_own, xt_own, x32, perm, lab_c = pl.pallas_call(
            prep_kernel,
            out_shape=[shape((tokens, dim), b16), shape((tokens, dim), b16), shape((dim, tokens), b16),
                       shape((tokens, dim), f32), shape((tokens, tokens), b16), shape((1, tokens), f32)],
            compiler_params=params(),
            name="prep",
        )(hid_rows, mask_rows, digits.astype(b16), gain.reshape(1, dim))
        other32 = lax.ppermute(x32, 'dp', swap)
        count = jnp.sum(mask_rows)
        mask_c = (jnp.arange(tokens, dtype=jnp.int32)[None, :] < count.astype(jnp.int32)).astype(f32)
        base = lax.axis_index('tp') * vocab
        lab_own = lab_c.astype(jnp.int32) - base
        nt_own = pl.cdiv(count.astype(jnp.int32), TILE).reshape(1)

        row = whole((1, tokens))
        row2 = whole((2, tokens))
        flops = 2 * tokens * vocab * dim
        elems = vocab * tokens

        bv = 2048
        t_own, sums, picks = table_call(
            logits_kernel, vocab, bv,
            [blocks(bv, dim), whole((dim, tokens)), row],
            [blocks(bv, tokens), whole((8, tokens)), whole((8, tokens))],
            [shape((vocab, tokens), f32), shape((8, tokens), f32), shape((8, tokens), f32)], [],
            pl.CostEstimate(flops=flops, bytes_accessed=elems * 4 + vocab * dim * 2, transcendentals=2 * elems),
        )(nt_own, embed_table, xt_own, lab_own)

        stat = lax.psum(jnp.stack([jnp.sum(sums, axis=0), jnp.sum(picks, axis=0)]), 'tp')
        pack_own = jnp.concatenate([stat, mask_c, lab_c], axis=0)
        pack_other = lax.ppermute(pack_own, 'dp', swap)
        z_both, pick_both, mask_both, lab_both = [jnp.stack([pack_own[k], pack_other[k]]) for k in range(4)]
        live = mask_both > 0.0
        z_both = jnp.where(live, z_both, 1.0)
        tok_count = jnp.maximum(jnp.sum(mask_both), 1.0)
        mean_loss = jnp.sum(jnp.where(live, jnp.log(z_both) - SOFT_CAP * pick_both, 0.0)) / tok_count
        lz = jnp.log2(z_both)
        ts = mask_both / tok_count
        lab = lab_both.astype(jnp.int32) - base
        nt_both = pl.cdiv(jnp.sum(mask_both, axis=1).astype(jnp.int32), TILE)

        bx = 1024
        gxt = table_call(
            grad_x_kernel, vocab, bx,
            [blocks(bx, dim), blocks(bx, tokens), row, row, row], whole((dim, tokens)), shape((dim, tokens), f32),
            [pltpu.VMEM((dim, bx), b16), pltpu.VMEM((bx, tokens), b16)],
            pl.CostEstimate(flops=flops, bytes_accessed=elems * 4 + vocab * dim * 2, transcendentals=elems),
        )(nt_own, embed_table, t_own, lab_own, lz[0:1], ts[0:1])
        grad_xt = lax.psum(gxt, 'tp')

        x_other, xt_other = pl.pallas_call(
            other_kernel, out_shape=[shape((tokens, dim), b16), shape((dim, tokens), b16)],
            compiler_params=params(), name="prep_other",
        )(other32)

        ts_late, _ = lax.optimization_barrier((ts, gxt[0, 0]))
        bt = 1024
        grad_table = table_call(
            grad_table_kernel, vocab, bt,
            [blocks(bt, dim), blocks(bt, tokens), whole((dim, tokens)), whole((tokens, dim)), whole((tokens, dim)),
             row2, row2, row2],
            blocks(bt, dim), shape((vocab, dim), f32), [pltpu.VMEM((bt, tokens), b16)],
            pl.CostEstimate(flops=3 * flops, bytes_accessed=elems * 4 + vocab * dim * 6, transcendentals=3 * elems),
        )(nt_both, embed_table, t_own, xt_other, x_own, x_other, lab, lz, ts_late)

        _, norm_back = jax.vjp(norm_apply, hid_c, gain)
        grad_rows, grad_gain = norm_back(grad_xt.T)
        grad_rows = jnp.einsum('it,id->td', perm, grad_rows, preferred_element_type=f32).astype(b16)
        grad_gain = lax.psum(grad_gain, 'dp')
        return mean_loss, grad_rows.reshape(batch_rows, seq_len, dim), grad_gain, grad_table

    return jax.shard_map(local_step, mesh=mesh, in_specs=(P('dp', None, None), P(None), P('tp', None), P('dp', None), P('dp', None)), out_specs=(P(), P('dp', None, None), P(None), P('tp', None)), check_vma=False)
```

```python
import functools
import jax
import jax.numpy as jnp
from jax import lax
from jax.experimental import pallas as pl
from jax.experimental.pallas import tpu as pltpu
from jax.sharding import PartitionSpec as P

SOFT_CAP = 30.0
LOG2E = 1.4426950408889634
CAP2 = SOFT_CAP * LOG2E
VMEM_LIMIT = 60 * 1024 * 1024
TILE = 256


def norm_apply(hid_rows, gain32):
    h32 = hid_rows.astype(jnp.float32)
    inv_rms = lax.rsqrt(jnp.mean(h32 * h32, axis=-1, keepdims=True) + 1e-6)
    return h32 * inv_rms * (1.0 + gain32)


def chunks(total, size):
    return [(s, min(size, total - s)) for s in range(0, total, size)]


def widths_of(tokens):
    return (tokens - TILE, tokens) if tokens > TILE else (tokens,)


def per_width(n_tiles, tokens, body):
    for w in widths_of(tokens):
        fits = n_tiles * TILE <= tokens - TILE
        cond = True if tokens <= TILE else (fits if w < tokens else jnp.logical_not(fits))

        @pl.when(cond)
        def _():
            body(w)


def pieces(t_refs, n, nn):
    edge = t_refs[0].shape[1]
    out = []
    if n < edge:
        out.append((t_refs[0], slice(n, min(n + nn, edge)), slice(0, min(nn, edge - n)), False))
    if n + nn > edge:
        lo = max(n, edge)
        out.append((t_refs[1], slice(lo - edge, n + nn - edge), slice(lo - n, nn), True))
    return out


def row_hits(rows, cols, base, labels):
    ids = lax.broadcasted_iota(jnp.int32, (rows, cols), 0)
    return ids == (labels - base)


def prep_kernel(hid_ref, mask_ref, dig_ref, gain_ref, hc_ref, x_ref, xt_ref, x32_ref, perm_ref, lab_ref):
    tokens = hid_ref.shape[0]
    mask = mask_ref[...]
    src = lax.broadcasted_iota(jnp.int32, (tokens, tokens), 0)
    dst = lax.broadcasted_iota(jnp.int32, (tokens, tokens), 1)
    upto = jnp.where(src <= dst, 1.0, 0.0).astype(jnp.bfloat16)
    count = jnp.dot(jnp.broadcast_to(mask, (8, tokens)).astype(jnp.bfloat16), upto, preferred_element_type=jnp.float32)
    place = jnp.where(mask > 0.0, count[0:1, :] - 1.0, -1.0).astype(jnp.int32)
    perm_ref[...] = jnp.where(src == place, 1.0, 0.0).astype(jnp.bfloat16)
    hc_ref[...] = jnp.dot(perm_ref[...], hid_ref[...], preferred_element_type=jnp.float32).astype(jnp.bfloat16)
    digits = lax.dot_general(dig_ref[...], perm_ref[...], (((1,), (1,)), ((), ())), preferred_element_type=jnp.float32)
    lab_ref[...] = digits[0:1, :] + 64.0 * digits[1:2, :] + 4096.0 * digits[2:3, :]
    for m, mm in chunks(tokens, TILE):
        rows = slice(m, m + mm)
        x32 = norm_apply(hc_ref[rows, :], gain_ref[...])
        x = x32.astype(jnp.bfloat16)
        x32_ref[rows, :] = x32
        x_ref[rows, :] = x
        xt_ref[:, rows] = x.T


def other_kernel(x32_ref, x_ref, xt_ref):
    x = x32_ref[...].astype(jnp.bfloat16)
    x_ref[...] = x
    xt_ref[...] = x.T


def logits_kernel(nblk, bv, tail, nt_ref, e_ref, xt_ref, lab_ref, ta_ref, tb_ref, sum_ref, pick_ref):
    i = pl.program_id(0)
    tokens = xt_ref.shape[1]

    @pl.when(i == 0)
    def _():
        sum_ref[...] = jnp.zeros_like(sum_ref)
        pick_ref[...] = jnp.zeros_like(pick_ref)

    def body(rows, width):
        for n, nn in chunks(width, TILE):
            cols = slice(n, n + nn)
            z = jnp.dot(e_ref[:rows, :], xt_ref[:, cols], preferred_element_type=jnp.float32)
            t = jnp.tanh(z * (1.0 / SOFT_CAP))
            for ref, rc, zc, _ in pieces((ta_ref, tb_ref), n, nn):
                ref[:rows, rc] = t[:, zc]
            e = jnp.exp2(t * CAP2)
            sum_ref[:, cols] += jnp.sum(e.reshape(rows // 8, 8, nn), axis=0)
            hit = row_hits(rows, nn, i * bv, lab_ref[0:1, cols])
            pick_ref[:, cols] += jnp.sum(jnp.where(hit, t, 0.0).reshape(rows // 8, 8, nn), axis=0)

    @pl.when(i < nblk - 1)
    def _():
        per_width(nt_ref[0], tokens, functools.partial(body, bv))

    @pl.when(i == nblk - 1)
    def _():
        body(tail, tokens)


def grad_of(t, base, lab, lz, ts):
    p = jnp.exp2(t * CAP2 - lz)
    hit = row_hits(t.shape[0], t.shape[1], base, lab)
    return (jnp.where(hit, p - 1.0, p) * ts * (1.0 - t * t)).astype(jnp.bfloat16)


def own_grads(g_ref, t_refs, n_tiles, n, nn, rows, base, lab_ref, lz_ref, ts_ref):
    tokens = t_refs[0].shape[1] + t_refs[1].shape[1]
    for ref, rc, zc, last in pieces(t_refs, n, nn):
        cols = slice(n + zc.start, n + zc.stop)
        for m, mm in chunks(rows, 64):
            t = ref[m:m + mm, rc]
            if last:
                t = jnp.where(n_tiles * TILE > tokens - TILE, t, 0.0)
            g_ref[m:m + mm, cols] = grad_of(t, base + m, lab_ref[0:1, cols], lz_ref[0:1, cols], ts_ref[0:1, cols])


def grad_x_kernel(nblk, bv, tail, nt_ref, e_ref, ta_ref, tb_ref, lab_ref, lz_ref, ts_ref, gx_ref, et_ref, g_ref):
    i = pl.program_id(0)
    tokens = gx_ref.shape[1]

    @pl.when(i == 0)
    def _():
        gx_ref[...] = jnp.zeros_like(gx_ref)

    def body(rows, width):
        for m, mm in chunks(rows, 256):
            et_ref[:, m:m + mm] = e_ref[m:m + mm, :].T
        for n, nn in chunks(width, 512):
            cols = slice(n, n + nn)
            own_grads(g_ref, (ta_ref, tb_ref), nt_ref[0], n, nn, rows, i * bv, lab_ref, lz_ref, ts_ref)
            dim = gx_ref.shape[0]
            for d, dd in chunks(dim, dim if nn > TILE else dim // 2):
                gx_ref[d:d + dd, cols] += jnp.dot(
                    et_ref[d:d + dd, :rows], g_ref[:rows, cols], preferred_element_type=jnp.float32)

    @pl.when(i < nblk - 1)
    def _():
        per_width(nt_ref[0], tokens, functools.partial(body, bv))

    @pl.when(i == nblk - 1)
    def _():
        body(tail, tokens)


def grad_table_kernel(nblk, bv, tail, nt_ref, e_ref, ta_ref, tb_ref, xto_ref, xs_ref, xo_ref, lab_ref, lz_ref, ts_ref, de_ref, g_ref):
    i = pl.program_id(0)
    tokens = xto_ref.shape[1]

    def body(rows, width):
        for n, nn in chunks(width, TILE):
            cols = slice(n, n + nn)
            z = jnp.dot(e_ref[:rows, :], xto_ref[:, cols], preferred_element_type=jnp.float32)
            t = jnp.tanh(z * (1.0 / SOFT_CAP))
            g_ref[:rows, tokens + n:tokens + n + nn] = grad_of(
                t, i * bv, lab_ref[1:2, cols], lz_ref[1:2, cols], ts_ref[1:2, cols])
            own_grads(g_ref, (ta_ref, tb_ref), nt_ref[0], n, nn, rows, i * bv, lab_ref, lz_ref, ts_ref)
        de_ref[:rows, :] = (
            jnp.dot(g_ref[:rows, :width], xs_ref[:width, :], preferred_element_type=jnp.float32)
            + jnp.dot(g_ref[:rows, tokens:tokens + width], xo_ref[:width, :], preferred_element_type=jnp.float32))

    @pl.when(i < nblk - 1)
    def _():
        per_width(jnp.maximum(nt_ref[0], nt_ref[1]), tokens, functools.partial(body, bv))

    @pl.when(i == nblk - 1)
    def _():
        body(tail, tokens)


def stats_kernel(n_dp, n_tp, vocab, pack_ref, lz_ref, ts_ref, lab_ref, count_ref, loss_ref, got, send_sem, recv_sem):
    dp, tp = lax.axis_index('dp'), lax.axis_index('tp')
    me = dp * n_tp + tp
    far = [(a, b) for a in range(n_dp) for b in range(n_tp) if a or b]
    peer = lambda a, b: {'dp': lax.rem(dp + a, n_dp), 'tp': lax.rem(tp + b, n_tp)}
    barrier = pltpu.get_barrier_semaphore()
    for a, b in far:
        pl.semaphore_signal(barrier, inc=1, device_id=peer(a, b), device_id_type=pl.DeviceIdType.MESH)
    pl.semaphore_wait(barrier, len(far))
    copies = []
    for k, (a, b) in enumerate(far):
        copies.append(pltpu.make_async_remote_copy(
            src_ref=pack_ref, dst_ref=got.at[me], send_sem=send_sem.at[k], recv_sem=recv_sem.at[k],
            device_id=peer(a, b), device_id_type=pl.DeviceIdType.MESH))
        copies[-1].start()
    got[me] = pack_ref[...]
    for c in copies:
        c.wait()
    zs, picks, masks, labs = [], [], [], []
    for d in range(n_dp):
        rows = [got[d * n_tp + k] for k in range(n_tp)]
        total = functools.reduce(lambda u, v: u + v, rows)
        live = rows[0][2:3, :] > 0.0
        masks.append(rows[0][2:3, :])
        labs.append(rows[0][3:4, :])
        zs.append(jnp.where(live, jnp.log(jnp.where(live, total[0:1, :], 1.0)), 0.0))
        picks.append(jnp.where(live, SOFT_CAP * total[1:2, :], 0.0))
    counts = [jnp.sum(m, axis=1, keepdims=True) for m in masks]
    n = jnp.maximum(functools.reduce(lambda u, v: u + v, counts), 1.0)
    losses = [jnp.sum(z - p, axis=1, keepdims=True) for z, p in zip(zs, picks)]
    loss = functools.reduce(lambda u, v: u + v, losses) / n
    loss_ref[...] = jnp.broadcast_to(loss, loss_ref.shape)
    first = dp == 0
    for r in range(n_dp):
        def pick(v):
            return jnp.where(first, v[r], v[n_dp - 1 - r])

        lz_ref[r:r + 1, :] = pick(zs) * LOG2E
        ts_ref[r:r + 1, :] = pick(masks) / n
        lab_ref[r:r + 1, :] = pick(labs).astype(jnp.int32) - tp * vocab
        count_ref[r:r + 1, :] = jnp.broadcast_to(pick(counts), (1, count_ref.shape[1])).astype(jnp.int32)


def whole(shape):
    return pl.BlockSpec(shape, lambda *_: (0,) * len(shape))


def blocks(rows, cols):
    return pl.BlockSpec((rows, cols), lambda i, *_: (i, 0))


def parked(rows, cols, tokens):
    return pl.BlockSpec((rows, cols), lambda i, nt: (jnp.where(nt[0] * TILE > tokens - TILE, i, 0), 0))


def params(**kw):
    return pltpu.CompilerParams(vmem_limit_bytes=VMEM_LIMIT, **kw)


def table_call(kernel, vocab, rows, in_specs, out_specs, out_shape, scratch, cost):
    nblk = pl.cdiv(vocab, rows)
    tail = vocab - (nblk - 1) * rows
    return pl.pallas_call(
        functools.partial(kernel, nblk, rows, tail),
        grid_spec=pltpu.PrefetchScalarGridSpec(
            num_scalar_prefetch=1, grid=(nblk,), in_specs=in_specs, out_specs=out_specs, scratch_shapes=scratch),
        out_shape=out_shape,
        compiler_params=params(dimension_semantics=("arbitrary",)),
        cost_estimate=cost,
    )


def solution(mesh):
    n_dp, n_tp = mesh.shape['dp'], mesh.shape['tp']
    swap = [(i, n_dp - 1 - i) for i in range(n_dp)]

    def local_step(hidden, norm_w, embed_table, labels, loss_mask):
        batch_rows, seq_len, dim = hidden.shape
        vocab = embed_table.shape[0]
        tokens = batch_rows * seq_len
        hid_rows = hidden.reshape(tokens, dim)
        mask_rows = loss_mask.reshape(1, tokens).astype(jnp.float32)
        gain = norm_w.astype(jnp.float32)
        lab_rows = labels.reshape(tokens)
        digits = jnp.stack([lab_rows & 63, (lab_rows >> 6) & 63, lab_rows >> 12] + [jnp.zeros_like(lab_rows)] * 5)
        f32, b16 = jnp.float32, jnp.bfloat16
        shape = jax.ShapeDtypeStruct
        hid_c, x_own, xt_own, x32, perm, lab_c = pl.pallas_call(
            prep_kernel,
            out_shape=[shape((tokens, dim), b16), shape((tokens, dim), b16), shape((dim, tokens), b16),
                       shape((tokens, dim), f32), shape((tokens, tokens), b16), shape((1, tokens), f32)],
            compiler_params=params(),
            name="prep",
        )(hid_rows, mask_rows, digits.astype(b16), gain.reshape(1, dim))
        other32 = lax.ppermute(x32, 'dp', swap)
        count = jnp.sum(mask_rows)
        mask_c = (jnp.arange(tokens, dtype=jnp.int32)[None, :] < count.astype(jnp.int32)).astype(f32)
        base = lax.axis_index('tp') * vocab
        lab_own = jnp.broadcast_to(lab_c.astype(jnp.int32) - base, (8, tokens))
        nt_own = pl.cdiv(count.astype(jnp.int32), TILE).reshape(1)

        row = whole((8, tokens))
        edge = tokens - TILE
        flops = 2 * tokens * vocab * dim
        elems = vocab * tokens

        bv = 1024
        t_a, t_b, sums, picks = table_call(
            logits_kernel, vocab, bv,
            [blocks(bv, dim), whole((dim, tokens)), row],
            [blocks(bv, edge), parked(bv, TILE, tokens), row, row],
            [shape((vocab, edge), f32), shape((vocab, TILE), f32), shape((8, tokens), f32), shape((8, tokens), f32)], [],
            pl.CostEstimate(flops=flops, bytes_accessed=elems * 4 + vocab * dim * 2, transcendentals=2 * elems),
        )(nt_own, embed_table, xt_own, lab_own)

        pack = jnp.concatenate([jnp.sum(sums, axis=0, keepdims=True), jnp.sum(picks, axis=0, keepdims=True), mask_c, lab_c,
                                jnp.zeros((4, tokens), f32)], axis=0)
        n_dev = n_dp * n_tp
        lz, ts, lab, counts, loss = pl.pallas_call(
            functools.partial(stats_kernel, n_dp, n_tp, vocab),
            out_shape=[shape((8, tokens), f32), shape((8, tokens), f32), shape((8, tokens), jnp.int32),
                       shape((8, 128), jnp.int32), shape((8, 128), f32)],
            in_specs=[pl.BlockSpec(memory_space=pltpu.VMEM)],
            out_specs=[pl.BlockSpec(memory_space=pltpu.VMEM)] * 5,
            scratch_shapes=[pltpu.VMEM((n_dev, 8, tokens), f32), pltpu.SemaphoreType.DMA((n_dev - 1,)),
                            pltpu.SemaphoreType.DMA((n_dev - 1,))],
            compiler_params=params(collective_id=0, has_side_effects=True),
            name="stats",
        )(pack)
        mean_loss = loss[0, 0]
        nt_both = pl.cdiv(counts[0:2, 0], TILE)

        bx = 1024
        gxt = table_call(
            grad_x_kernel, vocab, bx,
            [blocks(bx, dim), blocks(bx, edge), parked(bx, TILE, tokens), row, row, row], whole((dim, tokens)), shape((dim, tokens), f32),
            [pltpu.VMEM((dim, bx), b16), pltpu.VMEM((bx, tokens), b16)],
            pl.CostEstimate(flops=flops, bytes_accessed=elems * 4 + vocab * dim * 2, transcendentals=elems),
        )(nt_own, embed_table, t_a, t_b, lab, lz, ts)
        grad_xt = lax.psum(gxt, 'tp')

        x_other, xt_other = pl.pallas_call(
            other_kernel, out_shape=[shape((tokens, dim), b16), shape((dim, tokens), b16)],
            compiler_params=params(), name="prep_other",
        )(other32)

        ts_late, _ = lax.optimization_barrier((ts, gxt[0, 0]))
        bt = 1024
        grad_table = table_call(
            grad_table_kernel, vocab, bt,
            [blocks(bt, dim), blocks(bt, edge), parked(bt, TILE, tokens), whole((dim, tokens)), whole((tokens, dim)),
             whole((tokens, dim)), row, row, row],
            blocks(bt, dim), shape((vocab, dim), f32), [pltpu.VMEM((bt, 2 * tokens), b16)],
            pl.CostEstimate(flops=3 * flops, bytes_accessed=elems * 4 + vocab * dim * 6, transcendentals=3 * elems),
        )(nt_both, embed_table, t_a, t_b, xt_other, x_own, x_other, lab, lz, ts_late)

        _, norm_back = jax.vjp(norm_apply, hid_c, gain)
        grad_rows, grad_gain = norm_back(grad_xt.T)
        grad_rows = jnp.einsum('it,id->td', perm, grad_rows, preferred_element_type=f32).astype(b16)
        grad_gain = lax.psum(grad_gain, 'dp')
        return mean_loss, grad_rows.reshape(batch_rows, seq_len, dim), grad_gain, grad_table

    return jax.shard_map(local_step, mesh=mesh, in_specs=(P('dp', None, None), P(None), P('tp', None), P('dp', None), P('dp', None)), out_specs=(P(), P('dp', None, None), P(None), P('tp', None)), check_vma=False)
```

```python
import functools
import jax
import jax.numpy as jnp
from jax import lax
from jax.experimental import pallas as pl
from jax.experimental.pallas import tpu as pltpu
from jax.sharding import PartitionSpec as P

SOFT_CAP = 30.0
LOG2E = 1.4426950408889634
CAP2 = SOFT_CAP * LOG2E
VMEM_LIMIT = 60 * 1024 * 1024
TILE = 256


def norm_apply(hid_rows, gain32):
    h32 = hid_rows.astype(jnp.float32)
    inv_rms = lax.rsqrt(jnp.mean(h32 * h32, axis=-1, keepdims=True) + 1e-6)
    return h32 * inv_rms * (1.0 + gain32)


def chunks(total, size):
    return [(s, min(size, total - s)) for s in range(0, total, size)]


def widths_of(tokens):
    return (tokens - TILE, tokens) if tokens > TILE else (tokens,)


def per_width(n_tiles, tokens, body):
    for w in widths_of(tokens):
        fits = n_tiles * TILE <= tokens - TILE
        cond = True if tokens <= TILE else (fits if w < tokens else jnp.logical_not(fits))

        @pl.when(cond)
        def _():
            body(w)


def pieces(t_refs, n, nn):
    edge = t_refs[0].shape[1]
    out = []
    if n < edge:
        out.append((t_refs[0], slice(n, min(n + nn, edge)), slice(0, min(nn, edge - n)), False))
    if n + nn > edge:
        lo = max(n, edge)
        out.append((t_refs[1], slice(lo - edge, n + nn - edge), slice(lo - n, nn), True))
    return out


def row_hits(rows, cols, base, labels):
    ids = lax.broadcasted_iota(jnp.int32, (rows, cols), 0)
    return ids == (labels - base)


def prep_kernel(hid_ref, mask_ref, dig_ref, gain_ref, hc_ref, xt_ref, x32_ref, perm_ref, lab_ref):
    tokens = hid_ref.shape[0]
    mask = mask_ref[...]
    src = lax.broadcasted_iota(jnp.int32, (tokens, tokens), 0)
    dst = lax.broadcasted_iota(jnp.int32, (tokens, tokens), 1)
    upto = jnp.where(src <= dst, 1.0, 0.0).astype(jnp.bfloat16)
    count = jnp.dot(jnp.broadcast_to(mask, (8, tokens)).astype(jnp.bfloat16), upto, preferred_element_type=jnp.float32)
    place = jnp.where(mask > 0.0, count[0:1, :] - 1.0, -1.0).astype(jnp.int32)
    perm_ref[...] = jnp.where(src == place, 1.0, 0.0).astype(jnp.bfloat16)
    hc_ref[...] = jnp.dot(perm_ref[...], hid_ref[...], preferred_element_type=jnp.float32).astype(jnp.bfloat16)
    digits = lax.dot_general(dig_ref[...], perm_ref[...], (((1,), (1,)), ((), ())), preferred_element_type=jnp.float32)
    lab_ref[...] = digits[0:1, :] + 64.0 * digits[1:2, :] + 4096.0 * digits[2:3, :]
    for m, mm in chunks(tokens, TILE):
        rows = slice(m, m + mm)
        x32 = norm_apply(hc_ref[rows, :], gain_ref[...])
        x32_ref[rows, :] = x32
        xt_ref[:, rows] = x32.astype(jnp.bfloat16).T


def other_kernel(x32_ref, xt_ref):
    xt_ref[...] = x32_ref[...].astype(jnp.bfloat16).T


def logits_kernel(nblk, bv, tail, nt_ref, e_ref, xt_ref, lab_ref, ta_ref, tb_ref, sum_ref, pick_ref):
    i = pl.program_id(0)
    tokens = xt_ref.shape[1]

    @pl.when(i == 0)
    def _():
        sum_ref[...] = jnp.zeros_like(sum_ref)
        pick_ref[...] = jnp.zeros_like(pick_ref)

    def body(rows, width):
        for m, mm in chunks(rows, 256):
            for n, nn in chunks(width, 512):
                cols = slice(n, n + nn)
                z = jnp.dot(e_ref[m:m + mm, :], xt_ref[:, cols], preferred_element_type=jnp.float32)
                t = jnp.tanh(z * (1.0 / SOFT_CAP))
                for ref, rc, zc, _ in pieces((ta_ref, tb_ref), n, nn):
                    ref[m:m + mm, rc] = t[:, zc]
                e = jnp.exp2(t * CAP2)
                sum_ref[:, cols] += jnp.sum(e.reshape(mm // 8, 8, nn), axis=0)
                hit = row_hits(mm, nn, i * bv + m, lab_ref[0:1, cols])
                pick_ref[:, cols] += jnp.sum(jnp.where(hit, t, 0.0).reshape(mm // 8, 8, nn), axis=0)

    @pl.when(i < nblk - 1)
    def _():
        per_width(nt_ref[0], tokens, functools.partial(body, bv))

    @pl.when(i == nblk - 1)
    def _():
        body(tail, tokens)


def grad_of(t, base, lab, lz, ts):
    p = jnp.exp2(t * CAP2 - lz)
    hit = row_hits(t.shape[0], t.shape[1], base, lab)
    return (jnp.where(hit, p - 1.0, p) * ts * (1.0 - t * t)).astype(jnp.bfloat16)


def own_grads(g_ref, t_refs, n_tiles, n, nn, rows, base, lab_ref, lz_ref, ts_ref):
    tokens = t_refs[0].shape[1] + t_refs[1].shape[1]
    for ref, rc, zc, last in pieces(t_refs, n, nn):
        cols = slice(n + zc.start, n + zc.stop)
        for m, mm in chunks(rows, 64):
            t = ref[m:m + mm, rc]
            if last:
                t = jnp.where(n_tiles * TILE > tokens - TILE, t, 0.0)
            g_ref[m:m + mm, cols] = grad_of(t, base + m, lab_ref[0:1, cols], lz_ref[0:1, cols], ts_ref[0:1, cols])


def grad_x_kernel(nblk, bv, tail, nt_ref, e_ref, ta_ref, tb_ref, lab_ref, lz_ref, ts_ref, gx_ref, et_ref, g_ref):
    i = pl.program_id(0)
    tokens = gx_ref.shape[1]

    @pl.when(i == 0)
    def _():
        gx_ref[...] = jnp.zeros_like(gx_ref)

    def body(rows, width):
        for m, mm in chunks(rows, 256):
            et_ref[:, m:m + mm] = e_ref[m:m + mm, :].T
        for n, nn in chunks(width, 512):
            cols = slice(n, n + nn)
            own_grads(g_ref, (ta_ref, tb_ref), nt_ref[0], n, nn, rows, i * bv, lab_ref, lz_ref, ts_ref)
            dim = gx_ref.shape[0]
            for d, dd in chunks(dim, dim if nn > TILE else dim // 2):
                gx_ref[d:d + dd, cols] += jnp.dot(
                    et_ref[d:d + dd, :rows], g_ref[:rows, cols], preferred_element_type=jnp.float32)

    @pl.when(i < nblk - 1)
    def _():
        per_width(nt_ref[0], tokens, functools.partial(body, bv))

    @pl.when(i == nblk - 1)
    def _():
        body(tail, tokens)


def grad_table_kernel(nblk, bv, tail, nt_ref, e_ref, ta_ref, tb_ref, xts_ref, xto_ref, lab_ref, lz_ref, ts_ref, de_ref, g_ref):
    i = pl.program_id(0)
    tokens = xto_ref.shape[1]

    def over_tokens(a, b):
        return lax.dot_general(a, b, (((1,), (1,)), ((), ())), preferred_element_type=jnp.float32)

    def body(rows, width):
        for n, nn in chunks(width, 512):
            cols = slice(n, n + nn)
            for m, mm in chunks(rows, 256):
                z = jnp.dot(e_ref[m:m + mm, :], xto_ref[:, cols], preferred_element_type=jnp.float32)
                t = jnp.tanh(z * (1.0 / SOFT_CAP))
                g_ref[m:m + mm, tokens + n:tokens + n + nn] = grad_of(
                    t, i * bv + m, lab_ref[1:2, cols], lz_ref[1:2, cols], ts_ref[1:2, cols])
            own_grads(g_ref, (ta_ref, tb_ref), nt_ref[0], n, nn, rows, i * bv, lab_ref, lz_ref, ts_ref)
        sides = [(xts_ref[:, :width], g_ref[:rows, :width]), (xto_ref[:, :width], g_ref[:rows, tokens:tokens + width])]
        if rows % 128 == 0:
            (xa, ga), (xb, gb) = sides
            de_ref[:rows, :] = (over_tokens(xa, ga) + over_tokens(xb, gb)).T
        else:
            (xa, ga), (xb, gb) = sides
            de_ref[:rows, :] = over_tokens(ga, xa) + over_tokens(gb, xb)

    @pl.when(i < nblk - 1)
    def _():
        per_width(jnp.maximum(nt_ref[0], nt_ref[1]), tokens, functools.partial(body, bv))

    @pl.when(i == nblk - 1)
    def _():
        body(tail, tokens)


def stats_kernel(n_dp, n_tp, vocab, pack_ref, lz_ref, ts_ref, lab_ref, count_ref, loss_ref, got, send_sem, recv_sem):
    dp, tp = lax.axis_index('dp'), lax.axis_index('tp')
    me = dp * n_tp + tp
    far = [(a, b) for a in range(n_dp) for b in range(n_tp) if a or b]
    peer = lambda a, b: {'dp': lax.rem(dp + a, n_dp), 'tp': lax.rem(tp + b, n_tp)}
    barrier = pltpu.get_barrier_semaphore()
    for a, b in far:
        pl.semaphore_signal(barrier, inc=1, device_id=peer(a, b), device_id_type=pl.DeviceIdType.MESH)
    pl.semaphore_wait(barrier, len(far))
    copies = []
    for k, (a, b) in enumerate(far):
        copies.append(pltpu.make_async_remote_copy(
            src_ref=pack_ref, dst_ref=got.at[me], send_sem=send_sem.at[k], recv_sem=recv_sem.at[k],
            device_id=peer(a, b), device_id_type=pl.DeviceIdType.MESH))
        copies[-1].start()
    got[me] = pack_ref[...]
    for c in copies:
        c.wait()
    zs, picks, masks, labs = [], [], [], []
    for d in range(n_dp):
        rows = [got[d * n_tp + k] for k in range(n_tp)]
        total = functools.reduce(lambda u, v: u + v, rows)
        live = rows[0][2:3, :] > 0.0
        masks.append(rows[0][2:3, :])
        labs.append(rows[0][3:4, :])
        zs.append(jnp.where(live, jnp.log(jnp.where(live, total[0:1, :], 1.0)), 0.0))
        picks.append(jnp.where(live, SOFT_CAP * total[1:2, :], 0.0))
    counts = [jnp.sum(m, axis=1, keepdims=True) for m in masks]
    n = jnp.maximum(functools.reduce(lambda u, v: u + v, counts), 1.0)
    losses = [jnp.sum(z - p, axis=1, keepdims=True) for z, p in zip(zs, picks)]
    loss = functools.reduce(lambda u, v: u + v, losses) / n
    loss_ref[...] = jnp.broadcast_to(loss, loss_ref.shape)
    first = dp == 0
    for r in range(n_dp):
        def pick(v):
            return jnp.where(first, v[r], v[n_dp - 1 - r])

        lz_ref[r:r + 1, :] = pick(zs) * LOG2E
        ts_ref[r:r + 1, :] = pick(masks) / n
        lab_ref[r:r + 1, :] = pick(labs).astype(jnp.int32) - tp * vocab
        count_ref[r:r + 1, :] = jnp.broadcast_to(pick(counts), (1, count_ref.shape[1])).astype(jnp.int32)


def whole(shape):
    return pl.BlockSpec(shape, lambda *_: (0,) * len(shape))


def blocks(rows, cols):
    return pl.BlockSpec((rows, cols), lambda i, *_: (i, 0))


def parked(rows, cols, tokens):
    return pl.BlockSpec((rows, cols), lambda i, nt: (jnp.where(nt[0] * TILE > tokens - TILE, i, 0), 0))


def params(**kw):
    return pltpu.CompilerParams(vmem_limit_bytes=VMEM_LIMIT, **kw)


def table_call(kernel, vocab, rows, in_specs, out_specs, out_shape, scratch, cost):
    nblk = pl.cdiv(vocab, rows)
    tail = vocab - (nblk - 1) * rows
    return pl.pallas_call(
        functools.partial(kernel, nblk, rows, tail),
        grid_spec=pltpu.PrefetchScalarGridSpec(
            num_scalar_prefetch=1, grid=(nblk,), in_specs=in_specs, out_specs=out_specs, scratch_shapes=scratch),
        out_shape=out_shape,
        compiler_params=params(dimension_semantics=("arbitrary",)),
        cost_estimate=cost,
    )


def solution(mesh):
    n_dp, n_tp = mesh.shape['dp'], mesh.shape['tp']
    swap = [(i, n_dp - 1 - i) for i in range(n_dp)]

    def local_step(hidden, norm_w, embed_table, labels, loss_mask):
        batch_rows, seq_len, dim = hidden.shape
        vocab = embed_table.shape[0]
        tokens = batch_rows * seq_len
        hid_rows = hidden.reshape(tokens, dim)
        mask_rows = loss_mask.reshape(1, tokens).astype(jnp.float32)
        gain = norm_w.astype(jnp.float32)
        lab_rows = labels.reshape(tokens)
        digits = jnp.stack([lab_rows & 63, (lab_rows >> 6) & 63, lab_rows >> 12] + [jnp.zeros_like(lab_rows)] * 5)
        f32, b16 = jnp.float32, jnp.bfloat16
        shape = jax.ShapeDtypeStruct
        hid_c, xt_own, x32, perm, lab_c = pl.pallas_call(
            prep_kernel,
            out_shape=[shape((tokens, dim), b16), shape((dim, tokens), b16), shape((tokens, dim), f32),
                       shape((tokens, tokens), b16), shape((1, tokens), f32)],
            compiler_params=params(),
            name="prep",
        )(hid_rows, mask_rows, digits.astype(b16), gain.reshape(1, dim))
        other32 = lax.ppermute(x32, 'dp', swap)
        count = jnp.sum(mask_rows)
        mask_c = (jnp.arange(tokens, dtype=jnp.int32)[None, :] < count.astype(jnp.int32)).astype(f32)
        base = lax.axis_index('tp') * vocab
        lab_own = jnp.broadcast_to(lab_c.astype(jnp.int32) - base, (8, tokens))
        nt_own = pl.cdiv(count.astype(jnp.int32), TILE).reshape(1)

        row = whole((8, tokens))
        edge = tokens - TILE
        flops = 2 * tokens * vocab * dim
        elems = vocab * tokens

        bv = 1024
        t_a, t_b, sums, picks = table_call(
            logits_kernel, vocab, bv,
            [blocks(bv, dim), whole((dim, tokens)), row],
            [blocks(bv, edge), parked(bv, TILE, tokens), row, row],
            [shape((vocab, edge), f32), shape((vocab, TILE), f32), shape((8, tokens), f32), shape((8, tokens), f32)], [],
            pl.CostEstimate(flops=flops, bytes_accessed=elems * 4 + vocab * dim * 2, transcendentals=2 * elems),
        )(nt_own, embed_table, xt_own, lab_own)

        pack = jnp.concatenate([jnp.sum(sums, axis=0, keepdims=True), jnp.sum(picks, axis=0, keepdims=True), mask_c, lab_c,
                                jnp.zeros((4, tokens), f32)], axis=0)
        n_dev = n_dp * n_tp
        lz, ts, lab, counts, loss = pl.pallas_call(
            functools.partial(stats_kernel, n_dp, n_tp, vocab),
            out_shape=[shape((8, tokens), f32), shape((8, tokens), f32), shape((8, tokens), jnp.int32),
                       shape((8, 128), jnp.int32), shape((8, 128), f32)],
            in_specs=[pl.BlockSpec(memory_space=pltpu.VMEM)],
            out_specs=[pl.BlockSpec(memory_space=pltpu.VMEM)] * 5,
            scratch_shapes=[pltpu.VMEM((n_dev, 8, tokens), f32), pltpu.SemaphoreType.DMA((n_dev - 1,)),
                            pltpu.SemaphoreType.DMA((n_dev - 1,))],
            compiler_params=params(collective_id=0, has_side_effects=True),
            name="stats",
        )(pack)
        mean_loss = loss[0, 0]
        nt_both = pl.cdiv(counts[0:2, 0], TILE)

        bx = 1024
        gxt = table_call(
            grad_x_kernel, vocab, bx,
            [blocks(bx, dim), blocks(bx, edge), parked(bx, TILE, tokens), row, row, row], whole((dim, tokens)), shape((dim, tokens), f32),
            [pltpu.VMEM((dim, bx), b16), pltpu.VMEM((bx, tokens), b16)],
            pl.CostEstimate(flops=flops, bytes_accessed=elems * 4 + vocab * dim * 2, transcendentals=elems),
        )(nt_own, embed_table, t_a, t_b, lab, lz, ts)
        grad_xt = lax.psum(gxt, 'tp')

        xt_other = pl.pallas_call(
            other_kernel, out_shape=shape((dim, tokens), b16),
            compiler_params=params(), name="prep_other",
        )(other32)

        ts_late, _ = lax.optimization_barrier((ts, gxt[0, 0]))
        bt = 1024
        grad_table = table_call(
            grad_table_kernel, vocab, bt,
            [blocks(bt, dim), blocks(bt, edge), parked(bt, TILE, tokens), whole((dim, tokens)), whole((dim, tokens)),
             row, row, row],
            blocks(bt, dim), shape((vocab, dim), f32), [pltpu.VMEM((bt, 2 * tokens), b16)],
            pl.CostEstimate(flops=3 * flops, bytes_accessed=elems * 4 + vocab * dim * 6, transcendentals=3 * elems),
        )(nt_both, embed_table, t_a, t_b, xt_own, xt_other, lab, lz, ts_late)

        _, norm_back = jax.vjp(norm_apply, hid_c, gain)
        grad_rows, grad_gain = norm_back(grad_xt.T)
        grad_rows = jnp.einsum('it,id->td', perm, grad_rows, preferred_element_type=f32).astype(b16)
        grad_gain = lax.psum(grad_gain, 'dp')
        return mean_loss, grad_rows.reshape(batch_rows, seq_len, dim), grad_gain, grad_table

    return jax.shard_map(local_step, mesh=mesh, in_specs=(P('dp', None, None), P(None), P('tp', None), P('dp', None), P('dp', None)), out_specs=(P(), P('dp', None, None), P(None), P('tp', None)), check_vma=False)
```

```python
import functools
import jax
import jax.numpy as jnp
from jax import lax
from jax.experimental import pallas as pl
from jax.experimental.pallas import tpu as pltpu
from jax.sharding import PartitionSpec as P

SOFT_CAP = 30.0
LOG2E = 1.4426950408889634
CAP2 = SOFT_CAP * LOG2E
VMEM_LIMIT = 60 * 1024 * 1024
TILE = 256


def norm_apply(hid_rows, gain32):
    h32 = hid_rows.astype(jnp.float32)
    inv_rms = lax.rsqrt(jnp.mean(h32 * h32, axis=-1, keepdims=True) + 1e-6)
    return h32 * inv_rms * (1.0 + gain32)


def norm_apply_t(hid_cols, gain32):
    h32 = hid_cols.astype(jnp.float32)
    inv_rms = lax.rsqrt(jnp.mean(h32 * h32, axis=0, keepdims=True) + 1e-6)
    return h32 * inv_rms * (1.0 + gain32[:, None])


def chunks(total, size):
    return [(s, min(size, total - s)) for s in range(0, total, size)]


def widths_of(tokens):
    return (tokens - TILE, tokens) if tokens > TILE else (tokens,)


def per_width(n_tiles, tokens, body):
    for w in widths_of(tokens):
        fits = n_tiles * TILE <= tokens - TILE
        cond = True if tokens <= TILE else (fits if w < tokens else jnp.logical_not(fits))

        @pl.when(cond)
        def _():
            body(w)


def pieces(t_refs, n, nn):
    edge = t_refs[0].shape[1]
    out = []
    if n < edge:
        out.append((t_refs[0], slice(n, min(n + nn, edge)), slice(0, min(nn, edge - n)), False))
    if n + nn > edge:
        lo = max(n, edge)
        out.append((t_refs[1], slice(lo - edge, n + nn - edge), slice(lo - n, nn), True))
    return out


def row_hits(rows, cols, base, labels):
    ids = lax.broadcasted_iota(jnp.int32, (rows, cols), 0)
    return ids == (labels - base)


def prep_kernel(hid_ref, mask_ref, dig_ref, gain_ref, hct_ref, xt_ref, x32_ref, perm_ref, lab_ref, hc_ref):
    tokens = hid_ref.shape[0]
    mask = mask_ref[...]
    src = lax.broadcasted_iota(jnp.int32, (tokens, tokens), 0)
    dst = lax.broadcasted_iota(jnp.int32, (tokens, tokens), 1)
    upto = jnp.where(src <= dst, 1.0, 0.0).astype(jnp.bfloat16)
    count = jnp.dot(jnp.broadcast_to(mask, (8, tokens)).astype(jnp.bfloat16), upto, preferred_element_type=jnp.float32)
    place = jnp.where(mask > 0.0, count[0:1, :] - 1.0, -1.0).astype(jnp.int32)
    perm_ref[...] = jnp.where(src == place, 1.0, 0.0).astype(jnp.bfloat16)
    hc_ref[...] = jnp.dot(perm_ref[...], hid_ref[...], preferred_element_type=jnp.float32).astype(jnp.bfloat16)
    digits = lax.dot_general(dig_ref[...], perm_ref[...], (((1,), (1,)), ((), ())), preferred_element_type=jnp.float32)
    lab_ref[...] = digits[0:1, :] + 64.0 * digits[1:2, :] + 4096.0 * digits[2:3, :]
    for m, mm in chunks(tokens, TILE):
        rows = slice(m, m + mm)
        x32 = norm_apply(hc_ref[rows, :], gain_ref[...])
        x32_ref[rows, :] = x32
        xt_ref[:, rows] = x32.astype(jnp.bfloat16).T
        hct_ref[:, rows] = hc_ref[rows, :].T


def other_kernel(x32_ref, xt_ref):
    xt_ref[...] = x32_ref[...].astype(jnp.bfloat16).T


def logits_kernel(nblk, bv, tail, nt_ref, e_ref, xt_ref, lab_ref, ta_ref, tb_ref, sum_ref, pick_ref):
    i = pl.program_id(0)
    tokens = xt_ref.shape[1]

    @pl.when(i == 0)
    def _():
        sum_ref[...] = jnp.zeros_like(sum_ref)
        pick_ref[...] = jnp.zeros_like(pick_ref)

    def body(rows, width):
        for m, mm in chunks(rows, 256):
            for n, nn in chunks(width, 512):
                cols = slice(n, n + nn)
                z = jnp.dot(e_ref[m:m + mm, :], xt_ref[:, cols], preferred_element_type=jnp.float32)
                t = jnp.tanh(z * (1.0 / SOFT_CAP))
                for ref, rc, zc, _ in pieces((ta_ref, tb_ref), n, nn):
                    ref[m:m + mm, rc] = t[:, zc]
                e = jnp.exp2(t * CAP2)
                sum_ref[:, cols] += jnp.sum(e.reshape(mm // 8, 8, nn), axis=0)
                hit = row_hits(mm, nn, i * bv + m, lab_ref[0:1, cols])
                pick_ref[:, cols] += jnp.sum(jnp.where(hit, t, 0.0).reshape(mm // 8, 8, nn), axis=0)

    @pl.when(i < nblk - 1)
    def _():
        per_width(nt_ref[0], tokens, functools.partial(body, bv))

    @pl.when(i == nblk - 1)
    def _():
        body(tail, tokens)


def grad_of(t, base, lab, lz, ts):
    p = jnp.exp2(t * CAP2 - lz)
    hit = row_hits(t.shape[0], t.shape[1], base, lab)
    return (jnp.where(hit, p - 1.0, p) * ts * (1.0 - t * t)).astype(jnp.bfloat16)


def own_grads(g_ref, t_refs, n_tiles, n, nn, rows, base, lab_ref, lz_ref, ts_ref):
    tokens = t_refs[0].shape[1] + t_refs[1].shape[1]
    for ref, rc, zc, last in pieces(t_refs, n, nn):
        cols = slice(n + zc.start, n + zc.stop)
        for m, mm in chunks(rows, 64):
            t = ref[m:m + mm, rc]
            if last:
                t = jnp.where(n_tiles * TILE > tokens - TILE, t, 0.0)
            g_ref[m:m + mm, cols] = grad_of(t, base + m, lab_ref[0:1, cols], lz_ref[0:1, cols], ts_ref[0:1, cols])


def grad_x_kernel(nblk, bv, tail, nt_ref, e_ref, ta_ref, tb_ref, lab_ref, lz_ref, ts_ref, gx_ref, et_ref, g_ref):
    i = pl.program_id(0)
    tokens = gx_ref.shape[1]

    @pl.when(i == 0)
    def _():
        gx_ref[...] = jnp.zeros_like(gx_ref)

    def body(rows, width):
        for m, mm in chunks(rows, 256):
            et_ref[:, m:m + mm] = e_ref[m:m + mm, :].T
        for n, nn in chunks(width, 512):
            cols = slice(n, n + nn)
            own_grads(g_ref, (ta_ref, tb_ref), nt_ref[0], n, nn, rows, i * bv, lab_ref, lz_ref, ts_ref)
            dim = gx_ref.shape[0]
            for d, dd in chunks(dim, dim if nn > TILE else dim // 2):
                gx_ref[d:d + dd, cols] += jnp.dot(
                    et_ref[d:d + dd, :rows], g_ref[:rows, cols], preferred_element_type=jnp.float32)

    @pl.when(i < nblk - 1)
    def _():
        per_width(nt_ref[0], tokens, functools.partial(body, bv))

    @pl.when(i == nblk - 1)
    def _():
        body(tail, tokens)


def grad_table_kernel(nblk, bv, tail, nt_ref, e_ref, ta_ref, tb_ref, xts_ref, xto_ref, lab_ref, lz_ref, ts_ref, de_ref, g_ref):
    i = pl.program_id(0)
    tokens = xto_ref.shape[1]

    def over_tokens(a, b):
        return lax.dot_general(a, b, (((1,), (1,)), ((), ())), preferred_element_type=jnp.float32)

    def body(rows, own, other):
        for n, nn in chunks(max(own, other), 512):
            nn = min(n + nn, other) - n
            cols = slice(n, n + nn)
            for m, mm in chunks(rows, 256) if nn > 0 else ():
                z = jnp.dot(e_ref[m:m + mm, :], xto_ref[:, cols], preferred_element_type=jnp.float32)
                t = jnp.tanh(z * (1.0 / SOFT_CAP))
                g_ref[m:m + mm, tokens + n:tokens + n + nn] = grad_of(
                    t, i * bv + m, lab_ref[1:2, cols], lz_ref[1:2, cols], ts_ref[1:2, cols])
            nn = min(n + 512, own) - n
            if nn > 0:
                own_grads(g_ref, (ta_ref, tb_ref), nt_ref[0], n, nn, rows, i * bv, lab_ref, lz_ref, ts_ref)
        sides = [(xts_ref[:, :own], g_ref[:rows, :own]), (xto_ref[:, :other], g_ref[:rows, tokens:tokens + other])]
        if rows % 128 == 0:
            (xa, ga), (xb, gb) = sides
            de_ref[:rows, :] = (over_tokens(xa, ga) + over_tokens(xb, gb)).T
        else:
            (xa, ga), (xb, gb) = sides
            de_ref[:rows, :] = over_tokens(ga, xa) + over_tokens(gb, xb)

    @pl.when(i < nblk - 1)
    def _():
        per_width(nt_ref[0], tokens, lambda own: per_width(nt_ref[1], tokens, functools.partial(body, bv, own)))

    @pl.when(i == nblk - 1)
    def _():
        body(tail, tokens, tokens)


def stats_kernel(n_dp, n_tp, vocab, pack_ref, lz_ref, ts_ref, lab_ref, count_ref, loss_ref, got, send_sem, recv_sem):
    dp, tp = lax.axis_index('dp'), lax.axis_index('tp')
    me = dp * n_tp + tp
    far = [(a, b) for a in range(n_dp) for b in range(n_tp) if a or b]
    peer = lambda a, b: {'dp': lax.rem(dp + a, n_dp), 'tp': lax.rem(tp + b, n_tp)}
    barrier = pltpu.get_barrier_semaphore()
    for a, b in far:
        pl.semaphore_signal(barrier, inc=1, device_id=peer(a, b), device_id_type=pl.DeviceIdType.MESH)
    pl.semaphore_wait(barrier, len(far))
    copies = []
    for k, (a, b) in enumerate(far):
        copies.append(pltpu.make_async_remote_copy(
            src_ref=pack_ref, dst_ref=got.at[me], send_sem=send_sem.at[k], recv_sem=recv_sem.at[k],
            device_id=peer(a, b), device_id_type=pl.DeviceIdType.MESH))
        copies[-1].start()
    got[me] = pack_ref[...]
    for c in copies:
        c.wait()
    zs, picks, masks, labs = [], [], [], []
    for d in range(n_dp):
        rows = [got[d * n_tp + k] for k in range(n_tp)]
        total = functools.reduce(lambda u, v: u + v, rows)
        live = rows[0][2:3, :] > 0.0
        masks.append(rows[0][2:3, :])
        labs.append(rows[0][3:4, :])
        zs.append(jnp.where(live, jnp.log(jnp.where(live, total[0:1, :], 1.0)), 0.0))
        picks.append(jnp.where(live, SOFT_CAP * total[1:2, :], 0.0))
    counts = [jnp.sum(m, axis=1, keepdims=True) for m in masks]
    n = jnp.maximum(functools.reduce(lambda u, v: u + v, counts), 1.0)
    losses = [jnp.sum(z - p, axis=1, keepdims=True) for z, p in zip(zs, picks)]
    loss = functools.reduce(lambda u, v: u + v, losses) / n
    loss_ref[...] = jnp.broadcast_to(loss, loss_ref.shape)
    first = dp == 0
    for r in range(n_dp):
        def pick(v):
            return jnp.where(first, v[r], v[n_dp - 1 - r])

        lz_ref[r:r + 1, :] = pick(zs) * LOG2E
        ts_ref[r:r + 1, :] = pick(masks) / n
        lab_ref[r:r + 1, :] = pick(labs).astype(jnp.int32) - tp * vocab
        count_ref[r:r + 1, :] = jnp.broadcast_to(pick(counts), (1, count_ref.shape[1])).astype(jnp.int32)


def whole(shape):
    return pl.BlockSpec(shape, lambda *_: (0,) * len(shape))


def blocks(rows, cols):
    return pl.BlockSpec((rows, cols), lambda i, *_: (i, 0))


def parked(rows, cols, tokens):
    return pl.BlockSpec((rows, cols), lambda i, nt: (jnp.where(nt[0] * TILE > tokens - TILE, i, 0), 0))


def params(**kw):
    return pltpu.CompilerParams(vmem_limit_bytes=VMEM_LIMIT, **kw)


def table_call(kernel, vocab, rows, in_specs, out_specs, out_shape, scratch, cost):
    nblk = pl.cdiv(vocab, rows)
    tail = vocab - (nblk - 1) * rows
    return pl.pallas_call(
        functools.partial(kernel, nblk, rows, tail),
        grid_spec=pltpu.PrefetchScalarGridSpec(
            num_scalar_prefetch=1, grid=(nblk,), in_specs=in_specs, out_specs=out_specs, scratch_shapes=scratch),
        out_shape=out_shape,
        compiler_params=params(dimension_semantics=("arbitrary",)),
        cost_estimate=cost,
    )


def solution(mesh):
    n_dp, n_tp = mesh.shape['dp'], mesh.shape['tp']
    swap = [(i, n_dp - 1 - i) for i in range(n_dp)]

    def local_step(hidden, norm_w, embed_table, labels, loss_mask):
        batch_rows, seq_len, dim = hidden.shape
        vocab = embed_table.shape[0]
        tokens = batch_rows * seq_len
        hid_rows = hidden.reshape(tokens, dim)
        mask_rows = loss_mask.reshape(1, tokens).astype(jnp.float32)
        gain = norm_w.astype(jnp.float32)
        lab_rows = labels.reshape(tokens)
        digits = jnp.stack([lab_rows & 63, (lab_rows >> 6) & 63, lab_rows >> 12] + [jnp.zeros_like(lab_rows)] * 5)
        f32, b16 = jnp.float32, jnp.bfloat16
        shape = jax.ShapeDtypeStruct
        hid_ct, xt_own, x32, perm, lab_c = pl.pallas_call(
            prep_kernel,
            out_shape=[shape((dim, tokens), b16), shape((dim, tokens), b16), shape((tokens, dim), f32),
                       shape((tokens, tokens), b16), shape((1, tokens), f32)],
            scratch_shapes=[pltpu.VMEM((tokens, dim), b16)],
            compiler_params=params(),
            name="prep",
        )(hid_rows, mask_rows, digits.astype(b16), gain.reshape(1, dim))
        other32 = lax.ppermute(x32, 'dp', swap)
        count = jnp.sum(mask_rows)
        mask_c = (jnp.arange(tokens, dtype=jnp.int32)[None, :] < count.astype(jnp.int32)).astype(f32)
        base = lax.axis_index('tp') * vocab
        lab_own = jnp.broadcast_to(lab_c.astype(jnp.int32) - base, (8, tokens))
        nt_own = pl.cdiv(count.astype(jnp.int32), TILE).reshape(1)

        row = whole((8, tokens))
        edge = tokens - TILE
        flops = 2 * tokens * vocab * dim
        elems = vocab * tokens

        bv = 1024
        t_a, t_b, sums, picks = table_call(
            logits_kernel, vocab, bv,
            [blocks(bv, dim), whole((dim, tokens)), row],
            [blocks(bv, edge), parked(bv, TILE, tokens), row, row],
            [shape((vocab, edge), f32), shape((vocab, TILE), f32), shape((8, tokens), f32), shape((8, tokens), f32)], [],
            pl.CostEstimate(flops=flops, bytes_accessed=elems * 4 + vocab * dim * 2, transcendentals=2 * elems),
        )(nt_own, embed_table, xt_own, lab_own)

        pack = jnp.concatenate([jnp.sum(sums, axis=0, keepdims=True), jnp.sum(picks, axis=0, keepdims=True), mask_c, lab_c,
                                jnp.zeros((4, tokens), f32)], axis=0)
        n_dev = n_dp * n_tp
        lz, ts, lab, counts, loss = pl.pallas_call(
            functools.partial(stats_kernel, n_dp, n_tp, vocab),
            out_shape=[shape((8, tokens), f32), shape((8, tokens), f32), shape((8, tokens), jnp.int32),
                       shape((8, 128), jnp.int32), shape((8, 128), f32)],
            in_specs=[pl.BlockSpec(memory_space=pltpu.VMEM)],
            out_specs=[pl.BlockSpec(memory_space=pltpu.VMEM)] * 5,
            scratch_shapes=[pltpu.VMEM((n_dev, 8, tokens), f32), pltpu.SemaphoreType.DMA((n_dev - 1,)),
                            pltpu.SemaphoreType.DMA((n_dev - 1,))],
            compiler_params=params(collective_id=0, has_side_effects=True),
            name="stats",
        )(pack)
        mean_loss = loss[0, 0]
        nt_both = pl.cdiv(counts[0:2, 0], TILE)

        bx = 1024
        gxt = table_call(
            grad_x_kernel, vocab, bx,
            [blocks(bx, dim), blocks(bx, edge), parked(bx, TILE, tokens), row, row, row], whole((dim, tokens)), shape((dim, tokens), f32),
            [pltpu.VMEM((dim, bx), b16), pltpu.VMEM((bx, tokens), b16)],
            pl.CostEstimate(flops=flops, bytes_accessed=elems * 4 + vocab * dim * 2, transcendentals=elems),
        )(nt_own, embed_table, t_a, t_b, lab, lz, ts)
        grad_xt = lax.psum(gxt, 'tp')

        xt_other = pl.pallas_call(
            other_kernel, out_shape=shape((dim, tokens), b16),
            compiler_params=params(), name="prep_other",
        )(other32)

        ts_late, _ = lax.optimization_barrier((ts, gxt[0, 0]))
        bt = 1024
        grad_table = table_call(
            grad_table_kernel, vocab, bt,
            [blocks(bt, dim), blocks(bt, edge), parked(bt, TILE, tokens), whole((dim, tokens)), whole((dim, tokens)),
             row, row, row],
            blocks(bt, dim), shape((vocab, dim), f32), [pltpu.VMEM((bt, 2 * tokens), b16)],
            pl.CostEstimate(flops=3 * flops, bytes_accessed=elems * 4 + vocab * dim * 6, transcendentals=3 * elems),
        )(nt_both, embed_table, t_a, t_b, xt_own, xt_other, lab, lz, ts_late)

        _, norm_back = jax.vjp(norm_apply_t, hid_ct, gain)
        grad_cols, grad_gain = norm_back(grad_xt)
        grad_rows = jnp.einsum('it,di->td', perm, grad_cols, preferred_element_type=f32).astype(b16)
        grad_gain = lax.psum(grad_gain, 'dp')
        return mean_loss, grad_rows.reshape(batch_rows, seq_len, dim), grad_gain, grad_table

    return jax.shard_map(local_step, mesh=mesh, in_specs=(P('dp', None, None), P(None), P('tp', None), P('dp', None), P('dp', None)), out_specs=(P(), P('dp', None, None), P(None), P('tp', None)), check_vma=False)
```
